256 devices in a mesh: node: 8 (over y_lo, x), space: 32 (over z, y_hi, core).
Axes of the slice: x: 4, y: 4 (y_hi: 2, y_lo: 2; y = y_hi * 2 + y_lo), z: 8, core: 2. Of those that a mesh axis runs over, the one named last changes fastest.
Arguments:
- initial: float32 [2, 2048, 4096], P(None, 'space'), may hold values from 0 to 1
- sections: float32 [8, 2, 2048, 4096], P('node', None, 'space'), may hold values from 0 to 1
- feed_rate: float32 [2048, 4096], P('space'), may hold values from 0.02 to 0.12
- kill_rate: float32 [2048, 4096], P('space'), may hold values from 0.04 to 0.12
Outputs:
- new_sections: float32 [8, 2, 2048, 4096], P('node', None, 'space')
- residual_max: float32 [], replicated
The draws below stay inside these ranges and needn't reach their ends.
All inputs are finite; a program needn't handle non-finite values.
Results may differ from the reference program's by a relative error of at most 0.000094.
Values sent between devices are 32-bit elements; how exact they have to be, the bound alone decides.
A program may use at most 64 MiB of HBM per device.

```python
import math
import jax
import jax.numpy as jnp
import numpy as np
from jax import lax

NY = 4096
SWEEPS = 6
M = 8
NX = 2048


def steps_of(key, extent, cuts, low, high):
    def one(position, shards_of):
        draws = jax.random.uniform(jax.random.fold_in(jax.random.fold_in(key, 6), position), (shards_of,), jnp.float32, low / len(cuts), high / len(cuts))
        return jnp.repeat(jnp.exp(draws), extent[position] // shards_of).reshape((-1,) + (1,) * (len(extent) - position - 1))

    level = one(*cuts[0])
    for cut in cuts[1:]:
        level = level * one(*cut)
    return level


def setup_inputs(seed: int = 0) -> dict:
    arg_keys = jax.random.split(jax.random.key(seed), 5)
    return {
        "initial": jnp.clip(1.0 * jax.random.uniform(arg_keys[0], (2, NX, NY), jnp.float32) ** steps_of(arg_keys[0], (2, NX, NY), ((1, 32),), -0.2, 0.2), 0.0, 1.0),
        "sections": jnp.clip(1.0 * jax.random.uniform(arg_keys[1], (M, 2, NX, NY), jnp.float32) ** steps_of(arg_keys[1], (M, 2, NX, NY), ((0, 8), (2, 32)), -0.2, 0.2), 0.0, 1.0),
        "feed_rate": jnp.clip(jnp.exp(math.log(0.12) - 1.7917595 * jax.random.uniform(arg_keys[2], (NX, NY), jnp.float32) ** steps_of(arg_keys[2], (NX, NY), ((0, 32),), -0.2, 0.2)), 0.02, 0.12),
        "kill_rate": jnp.clip(jnp.exp(math.log(0.12) - 1.0986123 * jax.random.uniform(arg_keys[3], (NX, NY), jnp.float32) ** steps_of(arg_keys[3], (NX, NY), ((0, 32),), -0.2, 0.2)), 0.04, 0.12),
    }


step_size = 4.0
diff_u = 1.0
diff_v = 0.5


def radau_target(order, value):
    before = 1.0
    current = value
    previous = 1.0
    for degree in range(1, order):
        following = ((2 * degree + 1) * value * current - degree * before) / (degree + 1)
        before = current
        current = following
    if order == 1:
        previous = 1.0
    else:
        previous = before
    return current - previous


def radau_table(total):
    grid_count = 20000
    roots_found = []
    left_value = -1.0
    left_target = radau_target(total, left_value)
    for step_index in range(1, grid_count):
        right_value = -1.0 + 2.0 * step_index / grid_count
        right_target = radau_target(total, right_value)
        if left_target * right_target < 0.0:
            lower = left_value
            upper = right_value
            lower_target = left_target
            for bisect_index in range(80):
                halfway = 0.5 * (lower + upper)
                halfway_target = radau_target(total, halfway)
                if lower_target * halfway_target <= 0.0:
                    upper = halfway
                else:
                    lower = halfway
                    lower_target = halfway_target
            roots_found.append(0.5 * (lower + upper))
        left_value = right_value
        left_target = right_target
    roots_found.append(1.0)
    points = [(value + 1.0) / 2.0 for value in roots_found]
    quad_rows = []
    for node_index in range(total):
        row_values = []
        for basis_index in range(total):
            coefs = [1.0]
            for other_index in range(total):
                if other_index != basis_index:
                    scale = 1.0 / (points[basis_index] - points[other_index])
                    shifted = [0.0] + coefs
                    widened = coefs + [0.0]
                    coefs = [(shifted[k] - points[other_index] * widened[k]) * scale for k in range(len(shifted))]
            integral = 0.0
            for power_index in range(len(coefs)):
                integral += coefs[power_index] * points[node_index] ** (power_index + 1) / (power_index + 1)
            row_values.append(integral)
        quad_rows.append(row_values)
    return np.array(points), np.array(quad_rows)


def neighbours(field):
    return (jnp.roll(field, -1, 2) + jnp.roll(field, 1, 2)) + (jnp.roll(field, -1, 3) + jnp.roll(field, 1, 3))


def reference(initial, sections, feed_rate, kill_rate):
    points, quad_matrix = radau_table(M)
    points = jnp.asarray(points, jnp.float32)
    quad_matrix = jnp.asarray(quad_matrix, jnp.float32)
    diffusivity = jnp.array([diff_u, diff_v], jnp.float32).reshape(1, 2, 1, 1)
    laplace = neighbours(sections) - 4.0 * sections
    implicit = diffusivity * laplace
    species_u = sections[:, 0]
    species_v = sections[:, 1]
    product = species_u * species_v * species_v
    reaction = jnp.stack((-product + feed_rate * (1.0 - species_u), product - (feed_rate + kill_rate) * species_v), axis=1)
    slopes = implicit + reaction
    summed = jnp.einsum("mj,jsxy->msxy", quad_matrix, slopes, precision=lax.Precision.HIGHEST)
    quadrature = initial[None] + step_size * summed
    residual_max = jnp.max(jnp.abs(quadrature - sections))
    node_step = (step_size * points).reshape(M, 1, 1, 1)
    right_side = quadrature - node_step * implicit
    coupling = node_step * diffusivity
    divisor = 4.0 * coupling + 1.0
    iterate = sections
    for sweep_index in range(SWEEPS):
        iterate = (right_side + coupling * neighbours(iterate)) / divisor
    return iterate, residual_max
```

```python
import functools

import jax
import jax.numpy as jnp
import numpy as np
from jax import lax
from jax.experimental import pallas as pl
from jax.experimental.pallas import tpu as pltpu
from jax.sharding import PartitionSpec as P

SWEEPS = 6
STEP_SIZE = 4.0
DIFFUSIVITY = (1.0, 0.5)
MESH = pl.DeviceIdType.MESH

TILES = 8
BLOCKS = 32
ROWS = 80
ORDER = (1, 6, 0, 7, 2, 5, 3, 4)
LAST = ORDER[-1]
GROUP = 16


def radau_target(order, value):
    before = 1.0
    current = value
    previous = 1.0
    for degree in range(1, order):
        following = ((2 * degree + 1) * value * current - degree * before) / (degree + 1)
        before = current
        current = following
    previous = before
    return current - previous


@functools.lru_cache(maxsize=None)
def radau_table(total):
    grid_count = 20000
    roots_found = []
    left_value = -1.0
    left_target = radau_target(total, left_value)
    for step_index in range(1, grid_count):
        right_value = -1.0 + 2.0 * step_index / grid_count
        right_target = radau_target(total, right_value)
        if left_target * right_target < 0.0:
            lower = left_value
            upper = right_value
            lower_target = left_target
            for _ in range(80):
                halfway = 0.5 * (lower + upper)
                halfway_target = radau_target(total, halfway)
                if lower_target * halfway_target <= 0.0:
                    upper = halfway
                else:
                    lower = halfway
                    lower_target = halfway_target
            roots_found.append(0.5 * (lower + upper))
        left_value = right_value
        left_target = right_target
    roots_found.append(1.0)
    points = [(value + 1.0) / 2.0 for value in roots_found]
    quad_rows = []
    for node_index in range(total):
        row_values = []
        for basis_index in range(total):
            coefs = [1.0]
            for other_index in range(total):
                if other_index != basis_index:
                    scale = 1.0 / (points[basis_index] - points[other_index])
                    shifted = [0.0] + coefs
                    widened = coefs + [0.0]
                    coefs = [
                        (shifted[k] - points[other_index] * widened[k]) * scale
                        for k in range(len(shifted))
                    ]
            integral = 0.0
            for power_index in range(len(coefs)):
                integral += (
                    coefs[power_index] * points[node_index] ** (power_index + 1) / (power_index + 1)
                )
            row_values.append(integral)
        quad_rows.append(row_values)
    return (np.array(points, np.float32), np.array(quad_rows, np.float32))


def kernel(
    sec_hbm, init_hbm, feed_hbm, kill_hbm,
    out, res_out,
    levels, init, feed, kill, slopes, gathered, mixed, summed, drift, right, partial,
    halo_out, halo_in, edge_out, edge_in, top, top_in, best, best_in,
    load_sem, field_sem,
    slope_send, slope_recv, mixed_send, mixed_recv,
    halo_send, halo_recv, edge_send, edge_recv,
    top_send, top_recv, best_send, best_recv, known_sem,
):
    node = lax.axis_index("node")
    space = lax.axis_index("space")
    points, quad = radau_table(8)

    def per_node(values):
        chosen = jnp.float32(values[0])
        for index in range(1, 8):
            chosen = jnp.where(node == index, jnp.float32(values[index]), chosen)
        return chosen

    steps = np.float32(STEP_SIZE) * points
    couplings = [steps * np.float32(d) for d in DIFFUSIVITY]
    divisors = [np.float32(4.0) * c + np.float32(1.0) for c in couplings]
    node_step = per_node(steps)
    inverse = [per_node((1.0 / d.astype(np.float64)).astype(np.float32)) for d in divisors]
    ratio = [
        per_node((c.astype(np.float64) / d.astype(np.float64)).astype(np.float32))
        for c, d in zip(couplings, divisors)
    ]

    def node_peer(i):
        y, x = node // 4, node % 4
        return (((y + i // 4) % 2) * 4 + (x + i % 4) % 4, space)

    def node_index(i):
        return node_peer(i)[0]

    def plane_peer(j):
        return (node_index(j % 8), (space // 4) * 4 + (space % 4 + j // 8) % 4)

    def deep_peer(i):
        return (node, (space // 4 + i) % 8 * 4 + space % 4)

    def next_peer(i):
        return (node, (space + i + 32) % 32)

    barrier = pltpu.get_barrier_semaphore()
    greeted = (
        [node_peer(i) for i in range(1, 8)]
        + [plane_peer(8 * i) for i in range(1, 4)]
        + [deep_peer(1), deep_peer(7), next_peer(1), next_peer(-1)]
    )
    loads = []
    for t in range(TILES):
        for s in range(2):
            loads.append(pltpu.make_async_copy(
                sec_hbm.at[s, t], levels.at[0, s, :, pl.ds(8 + 8 * t, 8), :], load_sem.at[t, s]
            ))
    fields = [
        pltpu.make_async_copy(feed_hbm, feed, field_sem.at[0]),
        pltpu.make_async_copy(kill_hbm, kill, field_sem.at[1]),
        pltpu.make_async_copy(init_hbm, init, field_sem.at[2]),
    ]
    for copy in loads:
        copy.start()
    for copy in fields:
        copy.start()
    for peer in greeted:
        pl.semaphore_signal(barrier, inc=1, device_id=peer, device_id_type=MESH)

    lane = lax.broadcasted_iota(jnp.int32, (8, 128), 1)
    row = lax.broadcasted_iota(jnp.int32, (8, 128), 0)

    def beside(before, centre, after):
        left = pltpu.roll(jnp.where(lane == 127, before, centre), 1, 1)
        rightward = pltpu.roll(jnp.where(lane == 0, after, centre), 127, 1)
        return rightward + left

    def centres(load, first, count):
        blocks = [(first + BLOCKS - 1) % BLOCKS]
        blocks += [first + i for i in range(count)]
        blocks += [(first + count) % BLOCKS]
        return [load(b) for b in blocks]

    for copy in loads:
        copy.wait()

    for s in range(2):
        flat = levels.at[0, s].reshape(BLOCKS * ROWS, 128)
        halo_out[0, s] = flat[pl.ds(8, BLOCKS, stride=ROWS), :]
        halo_out[1, s] = flat[pl.ds(71, BLOCKS, stride=ROWS), :]
    for copy in fields:
        copy.wait()

    def slope_tile(t):
        base = 8 + 8 * t

        def body(d, carry):
            first = d * 4
            found = []
            for s in range(2):
                line = centres(lambda b: levels[0, s, b, pl.ds(base, 8), :], first, 4)
                laps = []
                for q in range(4):
                    up = levels[0, s, first + q, pl.ds(base - 1, 8), :]
                    down = levels[0, s, first + q, pl.ds(base + 1, 8), :]
                    around = (down + up) + beside(line[q], line[q + 1], line[q + 2])
                    laps.append((line[q + 1], around - 4.0 * line[q + 1]))
                found.append(laps)
            for q in range(4):
                u, lap_u = found[0][q]
                v, lap_v = found[1][q]
                lap_v = 0.5 * lap_v
                grow = feed[t, first + q]
                both = grow + kill[t, first + q]
                product = u * v * v
                slopes[t, d, 0, q] = lap_u + (grow * (1.0 - u) - product)
                slopes[t, d, 1, q] = lap_v + (product - both * v)
                drift[t, d, 0, q] = node_step * lap_u
                drift[t, d, 1, q] = node_step * lap_v
            return carry

        lax.fori_loop(0, 8, body, 0)

    def exchange(source, target, t, send_sem, recv_sem):
        copies = []
        for i in range(1, 8):
            copy = pltpu.make_async_remote_copy(
                source.at[t, node_index(i)], target.at[t, node],
                send_sem, recv_sem.at[t], device_id=node_peer(i), device_id_type=MESH,
            )
            copy.start()
        target[t, node] = source[t, node]

    def arrived(target, t, recv_sem):
        part = target.at[t, pl.ds(0, 7)]
        pltpu.make_async_copy(part, part, recv_sem.at[t]).wait()

    def mix_tile(t):
        def body(piece, carry):
            s, q = piece // 4, piece % 4
            values = [gathered[t, j, s, q] for j in range(8)]
            for m in range(8):
                total = values[0] * float(STEP_SIZE * quad[m, 0])
                for j in range(1, 8):
                    total = total + values[j] * float(STEP_SIZE * quad[m, j])
                mixed[t, m, s, q] = total
            return carry

        lax.fori_loop(0, 8, body, 0)

    def right_tile(t, biggest):
        base = 8 + 8 * t

        def body(d, carry):
            for s in range(2):
                for q in range(4):
                    block = d * 4 + q
                    value = init[s, t, block] + summed[t, d, s, q]
                    here = levels[0, s, block, pl.ds(base, 8), :]
                    carry = jnp.maximum(carry, jnp.abs(value - here))
                    right[t + 1, s, block] = (value - drift[t, d, s, q]) * inverse[s]
            return carry

        return lax.fori_loop(0, 8, body, biggest)

    def sweep(level, t, extra=None):
        base = 8 + 8 * t
        for s in range(2):
            def body(g, carry):
                first = g * GROUP
                line = centres(lambda b: levels[level - 1, s, b, pl.ds(base, 8), :], first, GROUP)
                for i in range(GROUP):
                    block = first + i
                    up = levels[level - 1, s, block, pl.ds(base - 1, 8), :]
                    down = levels[level - 1, s, block, pl.ds(base + 1, 8), :]
                    around = (down + up) + beside(line[i], line[i + 1], line[i + 2])
                    if extra is not None:
                        beyond = jnp.broadcast_to(
                            edge_in[extra, level - 2, s, pl.ds(block, 1), :], (8, 128)
                        )
                        around = around + jnp.where(row == 7 * extra, beyond, 0.0)
                    value = right[t + 1, s, block] + ratio[s] * around
                    if isinstance(level, int) and level == SWEEPS:
                        out[s, t, block] = value
                    else:
                        levels[level, s, block, pl.ds(base, 8), :] = value
                return carry

            lax.fori_loop(0, BLOCKS // GROUP, body, 0)

    def response(level, t, extra):
        base = 8 if extra == 0 else 64
        beyond = 0 if extra == 0 else 72
        for s in range(2):
            def body(g, carry):
                first = g * GROUP
                if level == 1:
                    for i in range(GROUP):
                        near = levels[0, s, first + i, pl.ds(base + (-7 if extra == 0 else 7), 8), :]
                        levels[1, s, first + i, pl.ds(beyond, 8), :] = jnp.where(
                            row == (7 if extra == 0 else 0), ratio[s] * near, 0.0
                        )
                    return carry
                line = centres(lambda b: levels[level - 1, s, b, pl.ds(beyond, 8), :], first, GROUP)
                for i in range(GROUP):
                    block = first + i
                    if extra == 0:
                        down = levels[level - 1, s, block, pl.ds(beyond + 1, 8), :]
                        up = jnp.where(row == 0, 0.0, pltpu.roll(line[i + 1], 1, 0))
                    else:
                        up = levels[level - 1, s, block, pl.ds(beyond - 1, 8), :]
                        down = jnp.where(row == 7, 0.0, pltpu.roll(line[i + 1], 7, 0))
                    around = (down + up) + beside(line[i], line[i + 1], line[i + 2])
                    levels[level, s, block, pl.ds(beyond, 8), :] = ratio[s] * around
                return carry

            lax.fori_loop(0, BLOCKS // GROUP, body, 0)

    def send_edges():
        for e, t in ((0, 0), (1, 7)):
            for s in range(2):
                for k in range(1, SWEEPS):
                    def body(g, carry):
                        first = g * GROUP
                        if k == 1:
                            load = lambda b: levels[0, s, b, pl.ds(8 + 8 * t, 8), :]
                        else:
                            load = lambda b: partial[(k - 1) % 2, e, s, b]
                        line = centres(load, first, GROUP)
                        for i in range(GROUP):
                            centre = line[i + 1]
                            up = jnp.where(row == 0, 0.0, pltpu.roll(centre, 1, 0))
                            down = jnp.where(row == 7, 0.0, pltpu.roll(centre, 7, 0))
                            around = (down + up) + beside(line[i], centre, line[i + 2])
                            partial[k % 2, e, s, first + i] = (
                                right[t + 1, s, first + i] + ratio[s] * around
                            )
                        return carry

                    lax.fori_loop(0, BLOCKS // GROUP, body, 0)
                    flat = partial.at[k % 2, e, s].reshape(BLOCKS * 8, 128)
                    edge_out[e, k - 1, s] = flat[pl.ds(7 * e, BLOCKS, stride=8), :]

    def side_copies(source, target, send_sem, recv_sem):
        return [
            pltpu.make_async_remote_copy(
                source.at[e], target.at[1 - e], send_sem.at[e], recv_sem.at[1 - e],
                device_id=next_peer(2 * e - 1), device_id_type=MESH,
            )
            for e in range(2)
        ]

    halo_copies = side_copies(halo_out, halo_in, halo_send, halo_recv)
    edge_copies = side_copies(edge_out, edge_in, edge_send, edge_recv)

    slope_tile(ORDER[0])
    pl.semaphore_wait(barrier, len(greeted))
    for copy in halo_copies:
        copy.start()
    exchange(slopes, gathered, ORDER[0], slope_send, slope_recv)
    for peer in [plane_peer(8 * i) for i in range(1, 4)] + [deep_peer(1), deep_peer(7)]:
        pl.semaphore_signal(known_sem.at[0], inc=1, device_id=peer, device_id_type=MESH)
    slope_tile(ORDER[1])
    exchange(slopes, gathered, ORDER[1], slope_send, slope_recv)
    for copy in halo_copies:
        copy.wait_recv()
    for s in range(2):
        flat = levels.at[0, s].reshape(BLOCKS * ROWS, 128)
        flat[pl.ds(7, BLOCKS, stride=ROWS), :] = halo_in[0, s]
        flat[pl.ds(72, BLOCKS, stride=ROWS), :] = halo_in[1, s]
    for t in ORDER[2:]:
        slope_tile(t)
        exchange(slopes, gathered, t, slope_send, slope_recv)
    pl.semaphore_wait(known_sem.at[0], 5)
    for i in (2, 6):
        pl.semaphore_signal(known_sem.at[1], inc=1, device_id=deep_peer(i), device_id_type=MESH)

    for t in ORDER:
        arrived(gathered, t, slope_recv)
        mix_tile(t)
        exchange(mixed, summed, t, mixed_send, mixed_recv)
    pl.semaphore_wait(known_sem.at[1], 2)

    biggest = jnp.zeros((8, 128), jnp.float32)
    for t in ORDER[:-1]:
        arrived(summed, t, mixed_recv)
        biggest = right_tile(t, biggest)
        if t == ORDER[3]:
            send_edges()
            for copy in edge_copies:
                copy.start()

    def sweep_range(low, high):
        def one_level(level, carry):
            lax.fori_loop(low, high, lambda t, c: (sweep(level, t), c)[1], 0)
            return carry

        lax.fori_loop(1, SWEEPS, one_level, 0)

    def last_level(low, high):
        lax.fori_loop(low, high, lambda t, c: (sweep(SWEEPS, t), c)[1], 0)

    def early_level(level, carry):
        def one(i, c):
            t = i + (i + (TILES - 1 - LAST)) // (TILES - 1)
            sweep(level, t)
            return c

        lax.fori_loop(0, TILES - 1, one, 0)
        return carry

    lax.fori_loop(1, SWEEPS, early_level, 0)
    last_level(1, LAST - 1)
    last_level(LAST + 2, TILES - 1)

    arrived(summed, LAST, mixed_recv)
    biggest = right_tile(LAST, biggest)
    top[...] = jnp.max(biggest, axis=0, keepdims=True)
    top_copies = []
    for j in range(1, 32):
        copy = pltpu.make_async_remote_copy(
            top, top_in.at[j], top_send.at[j], top_recv.at[j],
            device_id=plane_peer(j), device_id_type=MESH,
        )
        copy.start()
        top_copies.append(copy)
    top_in[0] = top[...]

    sweep_range(LAST - 1, LAST + 2)
    last_level(LAST - 1, LAST + 2)

    for copy in top_copies:
        copy.wait_recv()
    best[...] = jnp.max(top_in[...], axis=0)
    best_copies = []
    for i in range(1, 8):
        copy = pltpu.make_async_remote_copy(
            best, best_in.at[i], best_send.at[i], best_recv.at[i],
            device_id=deep_peer(i), device_id_type=MESH,
        )
        copy.start()
        best_copies.append(copy)
    best_in[0] = best[...]

    for copy in edge_copies:
        copy.wait_recv()
    for level in range(1, SWEEPS + 1):
        for e, t in ((0, 0), (1, 7)):
            if level > 1:
                sweep(level, t, extra=e)
            if level < SWEEPS:
                response(level, -1 if e == 0 else 8, e)

    for copy in best_copies:
        copy.wait_recv()
    res_out[0, 0] = jnp.max(best_in[...])

    for source, sem in ((slopes, slope_send), (mixed, mixed_send)):
        part = source.at[:, pl.ds(0, 7)]
        pltpu.make_async_copy(part, part, sem).wait()
    for copy in halo_copies + edge_copies + top_copies + best_copies:
        copy.wait_send()


def shards(initial, sections, feed_rate, kill_rate):
    def tiled(array):
        lead = array.shape[:-2]
        n = len(lead)
        split = array.reshape(lead + (TILES, 8, BLOCKS, 128))
        return jnp.swapaxes(split, n + 1, n + 2)

    f32 = jnp.float32
    whole = (2, TILES, BLOCKS, 8, 128)
    parts = (TILES, 8, 2, 4, 8, 128)
    dma = pltpu.SemaphoreType.DMA
    out, biggest = pl.pallas_call(
        kernel,
        out_shape=(
            jax.ShapeDtypeStruct(whole, f32),
            jax.ShapeDtypeStruct((1, 1), f32),
        ),
        in_specs=[pl.BlockSpec(memory_space=pl.ANY)] * 4,
        out_specs=(pl.BlockSpec(memory_space=pltpu.VMEM), pl.BlockSpec(memory_space=pltpu.SMEM)),
        scratch_shapes=[
            pltpu.VMEM((SWEEPS, 2, BLOCKS, ROWS, 128), f32),
            pltpu.VMEM(whole, f32),
            pltpu.VMEM(whole[1:], f32),
            pltpu.VMEM(whole[1:], f32),
            pltpu.VMEM(parts, f32),
            pltpu.VMEM(parts, f32),
            pltpu.VMEM(parts, f32),
            pltpu.VMEM(parts, f32),
            pltpu.VMEM(parts, f32),
            pltpu.VMEM((TILES + 2, 2, BLOCKS, 8, 128), f32),
            pltpu.VMEM((2, 2, 2, BLOCKS, 8, 128), f32),
            pltpu.VMEM((2, 2, BLOCKS, 128), f32),
            pltpu.VMEM((2, 2, BLOCKS, 128), f32),
            pltpu.VMEM((2, SWEEPS - 1, 2, BLOCKS, 128), f32),
            pltpu.VMEM((2, SWEEPS - 1, 2, BLOCKS, 128), f32),
            pltpu.VMEM((1, 128), f32),
            pltpu.VMEM((32, 1, 128), f32),
            pltpu.VMEM((1, 128), f32),
            pltpu.VMEM((8, 1, 128), f32),
            dma((TILES, 2)),
            dma((3,)),
            dma,
            dma((TILES,)),
            dma,
            dma((TILES,)),
            dma((2,)),
            dma((2,)),
            dma((2,)),
            dma((2,)),
            dma((32,)),
            dma((32,)),
            dma((8,)),
            dma((8,)),
            pltpu.SemaphoreType.REGULAR((2,)),
        ],
        compiler_params=pltpu.CompilerParams(
            collective_id=0, has_side_effects=True, vmem_limit_bytes=56 * 1024 * 1024
        ),
    )(tiled(sections[0]), tiled(initial), tiled(feed_rate), tiled(kill_rate))
    new = jnp.swapaxes(out, 2, 3).reshape(sections.shape)
    return (new, biggest.reshape(()))


def solution(mesh):
    return jax.shard_map(
        shards,
        mesh=mesh,
        in_specs=(
            P(None, "space", None),
            P("node", None, "space", None),
            P("space", None),
            P("space", None),
        ),
        out_specs=(P("node", None, "space", None), P()),
        check_vma=False,
    )
```

```python
import functools

import jax
import jax.numpy as jnp
import numpy as np
from jax import lax
from jax.experimental import pallas as pl
from jax.experimental.pallas import tpu as pltpu
from jax.sharding import PartitionSpec as P

SWEEPS = 6
STEP_SIZE = 4.0
DIFFUSIVITY = (1.0, 0.5)
MESH = pl.DeviceIdType.MESH

TILES = 8
BLOCKS = 32
ROWS = 104
FIRST = 16
ORDER = (1, 6, 0, 7, 5, 4, 3, 2)
GROUP = 16


def radau_target(order, value):
    before = 1.0
    current = value
    previous = 1.0
    for degree in range(1, order):
        following = ((2 * degree + 1) * value * current - degree * before) / (degree + 1)
        before = current
        current = following
    previous = before
    return current - previous


@functools.lru_cache(maxsize=None)
def radau_table(total):
    grid_count = 20000
    roots_found = []
    left_value = -1.0
    left_target = radau_target(total, left_value)
    for step_index in range(1, grid_count):
        right_value = -1.0 + 2.0 * step_index / grid_count
        right_target = radau_target(total, right_value)
        if left_target * right_target < 0.0:
            lower = left_value
            upper = right_value
            lower_target = left_target
            for _ in range(80):
                halfway = 0.5 * (lower + upper)
                halfway_target = radau_target(total, halfway)
                if lower_target * halfway_target <= 0.0:
                    upper = halfway
                else:
                    lower = halfway
                    lower_target = halfway_target
            roots_found.append(0.5 * (lower + upper))
        left_value = right_value
        left_target = right_target
    roots_found.append(1.0)
    points = [(value + 1.0) / 2.0 for value in roots_found]
    quad_rows = []
    for node_index in range(total):
        row_values = []
        for basis_index in range(total):
            coefs = [1.0]
            for other_index in range(total):
                if other_index != basis_index:
                    scale = 1.0 / (points[basis_index] - points[other_index])
                    shifted = [0.0] + coefs
                    widened = coefs + [0.0]
                    coefs = [
                        (shifted[k] - points[other_index] * widened[k]) * scale
                        for k in range(len(shifted))
                    ]
            integral = 0.0
            for power_index in range(len(coefs)):
                integral += (
                    coefs[power_index] * points[node_index] ** (power_index + 1) / (power_index + 1)
                )
            row_values.append(integral)
        quad_rows.append(row_values)
    return (np.array(points, np.float32), np.array(quad_rows, np.float32))


def kernel(
    sec_hbm, init_hbm, feed_hbm, kill_hbm,
    out, res_out,
    levels, init, feed, kill, slopes, gathered, mixed, summed, drift, right, partial,
    halo_out, halo_in, edge_out, edge_in, top, top_in, best, best_in,
    load_sem, field_sem, init_sem,
    slope_send, slope_recv, mixed_send, mixed_recv,
    halo_send, halo_recv, edge_send, edge_recv,
    top_send, top_recv, best_send, best_recv, known_sem,
):
    node = lax.axis_index("node")
    space = lax.axis_index("space")
    points, quad = radau_table(8)

    def per_node(values):
        chosen = jnp.float32(values[0])
        for index in range(1, 8):
            chosen = jnp.where(node == index, jnp.float32(values[index]), chosen)
        return chosen

    steps = np.float32(STEP_SIZE) * points
    couplings = [steps * np.float32(d) for d in DIFFUSIVITY]
    divisors = [np.float32(4.0) * c + np.float32(1.0) for c in couplings]
    node_step = per_node(steps)
    inverse = [per_node((1.0 / d.astype(np.float64)).astype(np.float32)) for d in divisors]
    ratio = [
        per_node((c.astype(np.float64) / d.astype(np.float64)).astype(np.float32))
        for c, d in zip(couplings, divisors)
    ]

    def node_peer(i):
        y, x = node // 4, node % 4
        return (((y + i // 4) % 2) * 4 + (x + i % 4) % 4, space)

    def node_index(i):
        return node_peer(i)[0]

    def plane_peer(j):
        return (node_index(j % 8), (space // 4) * 4 + (space % 4 + j // 8) % 4)

    def deep_peer(i):
        return (node, (space // 4 + i) % 8 * 4 + space % 4)

    def next_peer(i):
        return (node, (space + i + 32) % 32)

    barrier = pltpu.get_barrier_semaphore()
    greeted = (
        [node_peer(i) for i in range(1, 8)]
        + [plane_peer(8 * i) for i in range(1, 4)]
        + [deep_peer(1), deep_peer(7), next_peer(1), next_peer(-1)]
    )
    loads = []
    for t in range(TILES):
        loads.append([
            pltpu.make_async_copy(
                sec_hbm.at[s, t], levels.at[0, s, :, pl.ds(FIRST + 8 * t, 8), :], load_sem.at[t, s]
            )
            for s in range(2)
        ])
    fields = [
        [
            pltpu.make_async_copy(feed_hbm.at[t], feed.at[t], field_sem.at[t, 0]),
            pltpu.make_async_copy(kill_hbm.at[t], kill.at[t], field_sem.at[t, 1]),
        ]
        for t in range(TILES)
    ]
    init_load = pltpu.make_async_copy(init_hbm, init, init_sem)
    started, waited = set(), set()

    def start_loads(t):
        for near in (t - 1, t, t + 1):
            if 0 <= near < TILES and near not in started:
                started.add(near)
                for copy in loads[near]:
                    copy.start()
        for copy in fields[t]:
            copy.start()

    def wait_loads(t):
        for near in (t - 1, t, t + 1):
            if 0 <= near < TILES and near not in waited:
                waited.add(near)
                for copy in loads[near]:
                    copy.wait()
        for copy in fields[t]:
            copy.wait()

    start_loads(ORDER[0])
    for peer in greeted:
        pl.semaphore_signal(barrier, inc=1, device_id=peer, device_id_type=MESH)
    for t in ORDER[1:]:
        start_loads(t)
    init_load.start()

    lane = lax.broadcasted_iota(jnp.int32, (8, 128), 1)
    row = lax.broadcasted_iota(jnp.int32, (8, 128), 0)

    def beside(before, centre, after):
        left = pltpu.roll(jnp.where(lane == 127, before, centre), 1, 1)
        rightward = pltpu.roll(jnp.where(lane == 0, after, centre), 127, 1)
        return rightward + left

    def centres(load, first, count):
        blocks = [(first + BLOCKS - 1) % BLOCKS]
        blocks += [first + i for i in range(count)]
        blocks += [(first + count) % BLOCKS]
        return [load(b) for b in blocks]

    def slope_tile(t):
        base = FIRST + 8 * t

        def body(d, carry):
            first = d * 4
            found = []
            for s in range(2):
                line = centres(lambda b: levels[0, s, b, pl.ds(base, 8), :], first, 4)
                laps = []
                for q in range(4):
                    up = levels[0, s, first + q, pl.ds(base - 1, 8), :]
                    down = levels[0, s, first + q, pl.ds(base + 1, 8), :]
                    around = (down + up) + beside(line[q], line[q + 1], line[q + 2])
                    laps.append((line[q + 1], around - 4.0 * line[q + 1]))
                found.append(laps)
            for q in range(4):
                u, lap_u = found[0][q]
                v, lap_v = found[1][q]
                lap_v = 0.5 * lap_v
                grow = feed[t, first + q]
                both = grow + kill[t, first + q]
                product = u * v * v
                slopes[t, d, 0, q] = lap_u + (grow * (1.0 - u) - product)
                slopes[t, d, 1, q] = lap_v + (product - both * v)
                drift[t, d, 0, q] = node_step * lap_u
                drift[t, d, 1, q] = node_step * lap_v
            return carry

        lax.fori_loop(0, 8, body, 0)

    def exchange(source, target, t, send_sem, recv_sem):
        copies = []
        for i in range(1, 8):
            copy = pltpu.make_async_remote_copy(
                source.at[t, node_index(i)], target.at[t, node],
                send_sem, recv_sem.at[t], device_id=node_peer(i), device_id_type=MESH,
            )
            copy.start()
        target[t, node] = source[t, node]

    def arrived(target, t, recv_sem):
        part = target.at[t, pl.ds(0, 7)]
        pltpu.make_async_copy(part, part, recv_sem.at[t]).wait()

    def mix_tile(t):
        def body(piece, carry):
            s, q = piece // 4, piece % 4
            values = [gathered[t, j, s, q] for j in range(8)]
            for m in range(8):
                total = values[0] * float(STEP_SIZE * quad[m, 0])
                for j in range(1, 8):
                    total = total + values[j] * float(STEP_SIZE * quad[m, j])
                mixed[t, m, s, q] = total
            return carry

        lax.fori_loop(0, 8, body, 0)

    def right_tile(t, biggest):
        base = FIRST + 8 * t

        def body(d, carry):
            for s in range(2):
                for q in range(4):
                    block = d * 4 + q
                    value = init[s, t, block] + summed[t, d, s, q]
                    here = levels[0, s, block, pl.ds(base, 8), :]
                    carry = jnp.maximum(carry, jnp.abs(value - here))
                    right[t + 1, s, block] = (value - drift[t, d, s, q]) * inverse[s]
            return carry

        return lax.fori_loop(0, 8, body, biggest)

    def sweep(level, t, side=None):
        base = pl.multiple_of(FIRST + 8 * t, 8)
        for s in range(2):
            line = centres(lambda b: levels[level - 1, s, b, pl.ds(base, 8), :], 0, BLOCKS)
            for b in range(BLOCKS):
                up = levels[level - 1, s, b, pl.ds(base - 1, 8), :]
                down = levels[level - 1, s, b, pl.ds(base + 1, 8), :]
                around = (down + up) + beside(line[b], line[b + 1], line[b + 2])
                if side is not None:
                    beyond = jnp.broadcast_to(edge_in[side, level - 2, s, pl.ds(b, 1), :], (8, 128))
                    around = around + jnp.where(row == 7 * side, beyond, 0.0)
                value = right[t + 1, s, b] + ratio[s] * around
                if level == SWEEPS:
                    out[s, t, b] = value
                else:
                    levels[level, s, b, pl.ds(base, 8), :] = value

    def response(level, side):
        base = pl.multiple_of(FIRST - 8 + 72 * side, 8)
        for s in range(2):
            if level == 1:
                for b in range(BLOCKS):
                    near = levels[0, s, b, pl.ds(base + 1 - 2 * side, 8), :]
                    levels[1, s, b, pl.ds(base, 8), :] = jnp.where(
                        row == 7 - 7 * side, ratio[s] * near, 0.0
                    )
                continue
            line = centres(lambda b: levels[level - 1, s, b, pl.ds(base, 8), :], 0, BLOCKS)
            for b in range(BLOCKS):
                up = levels[level - 1, s, b, pl.ds(base - 1, 8), :]
                down = levels[level - 1, s, b, pl.ds(base + 1, 8), :]
                around = (down + up) + beside(line[b], line[b + 1], line[b + 2])
                levels[level, s, b, pl.ds(base, 8), :] = ratio[s] * around

    def repeat(low, high, run):
        def body(t, carry):
            run(t)
            return carry

        lax.fori_loop(low, high, body, 0)

    def sweep_all(low, high, last_low, last_high):
        for level in range(1, SWEEPS):
            repeat(low, high, functools.partial(sweep, level))
        if last_high > last_low:
            repeat(last_low, last_high, functools.partial(sweep, SWEEPS))

    def send_edges():
        for e, t in ((0, 0), (1, 7)):
            for s in range(2):
                for k in range(1, SWEEPS):
                    def body(g, carry):
                        first = g * GROUP
                        if k == 1:
                            load = lambda b: levels[0, s, b, pl.ds(FIRST + 8 * t, 8), :]
                        else:
                            load = lambda b: partial[(k - 1) % 2, e, s, b]
                        line = centres(load, first, GROUP)
                        for i in range(GROUP):
                            centre = line[i + 1]
                            up = jnp.where(row == 0, 0.0, pltpu.roll(centre, 1, 0))
                            down = jnp.where(row == 7, 0.0, pltpu.roll(centre, 7, 0))
                            around = (down + up) + beside(line[i], centre, line[i + 2])
                            partial[k % 2, e, s, first + i] = (
                                right[t + 1, s, first + i] + ratio[s] * around
                            )
                        return carry

                    lax.fori_loop(0, BLOCKS // GROUP, body, 0)
                    flat = partial.at[k % 2, e, s].reshape(BLOCKS * 8, 128)
                    edge_out[e, k - 1, s] = flat[pl.ds(7 * e, BLOCKS, stride=8), :]

    def side_copies(source, target, send_sem, recv_sem):
        return [
            pltpu.make_async_remote_copy(
                source.at[e], target.at[1 - e], send_sem.at[e], recv_sem.at[1 - e],
                device_id=next_peer(2 * e - 1), device_id_type=MESH,
            )
            for e in range(2)
        ]

    halo_copies = side_copies(halo_out, halo_in, halo_send, halo_recv)
    edge_copies = side_copies(edge_out, edge_in, edge_send, edge_recv)

    wait_loads(ORDER[0])
    slope_tile(ORDER[0])
    pl.semaphore_wait(barrier, len(greeted))
    exchange(slopes, gathered, ORDER[0], slope_send, slope_recv)
    wait_loads(ORDER[1])
    for s in range(2):
        flat = levels.at[0, s].reshape(BLOCKS * ROWS, 128)
        halo_out[0, s] = flat[pl.ds(FIRST, BLOCKS, stride=ROWS), :]
        halo_out[1, s] = flat[pl.ds(FIRST + 63, BLOCKS, stride=ROWS), :]
    for copy in halo_copies:
        copy.start()
    for peer in [plane_peer(8 * i) for i in range(1, 4)] + [deep_peer(1), deep_peer(7)]:
        pl.semaphore_signal(known_sem.at[0], inc=1, device_id=peer, device_id_type=MESH)
    slope_tile(ORDER[1])
    exchange(slopes, gathered, ORDER[1], slope_send, slope_recv)
    for copy in halo_copies:
        copy.wait_recv()
    for s in range(2):
        flat = levels.at[0, s].reshape(BLOCKS * ROWS, 128)
        flat[pl.ds(FIRST - 1, BLOCKS, stride=ROWS), :] = halo_in[0, s]
        flat[pl.ds(FIRST + 64, BLOCKS, stride=ROWS), :] = halo_in[1, s]
    for t in ORDER[2:]:
        wait_loads(t)
        slope_tile(t)
        exchange(slopes, gathered, t, slope_send, slope_recv)
    pl.semaphore_wait(known_sem.at[0], 5)
    for i in (2, 6):
        pl.semaphore_signal(known_sem.at[1], inc=1, device_id=deep_peer(i), device_id_type=MESH)

    init_load.wait()
    for t in ORDER:
        arrived(gathered, t, slope_recv)
        mix_tile(t)
        exchange(mixed, summed, t, mixed_send, mixed_recv)
    pl.semaphore_wait(known_sem.at[1], 2)

    biggest = jnp.zeros((8, 128), jnp.float32)
    for index, t in enumerate(ORDER):
        arrived(summed, t, mixed_recv)
        biggest = right_tile(t, biggest)
        if index == 3:
            send_edges()
            for copy in edge_copies:
                copy.start()
        if index == 2:
            sweep_all(0, 2, 0, 0)
        if index == 4:
            sweep_all(5, 8, 6, 7)
        if index == 5:
            sweep_all(4, 6, 5, 6)
        if index == 6:
            sweep_all(3, 5, 4, 5)

    top[...] = jnp.max(biggest, axis=0, keepdims=True)
    top_copies = []
    for j in range(1, 32):
        copy = pltpu.make_async_remote_copy(
            top, top_in.at[j], top_send.at[j], top_recv.at[j],
            device_id=plane_peer(j), device_id_type=MESH,
        )
        copy.start()
        top_copies.append(copy)
    top_in[0] = top[...]

    sweep_all(1, 4, 1, 4)

    for copy in top_copies:
        copy.wait_recv()
    best[...] = jnp.max(top_in[...], axis=0)
    best_copies = []
    for i in range(1, 8):
        copy = pltpu.make_async_remote_copy(
            best, best_in.at[i], best_send.at[i], best_recv.at[i],
            device_id=deep_peer(i), device_id_type=MESH,
        )
        copy.start()
        best_copies.append(copy)
    best_in[0] = best[...]

    for copy in edge_copies:
        copy.wait_recv()
    for level in range(1, SWEEPS + 1):
        if level > 1:
            repeat(0, 2, lambda side: sweep(level, 7 * side, side))
        if level < SWEEPS:
            repeat(0, 2, functools.partial(response, level))

    for copy in best_copies:
        copy.wait_recv()
    res_out[0, 0] = jnp.max(best_in[...])

    for source, sem in ((slopes, slope_send), (mixed, mixed_send)):
        part = source.at[:, pl.ds(0, 7)]
        pltpu.make_async_copy(part, part, sem).wait()
    for copy in halo_copies + edge_copies + top_copies + best_copies:
        copy.wait_send()


def shards(initial, sections, feed_rate, kill_rate):
    def tiled(array):
        lead = array.shape[:-2]
        n = len(lead)
        split = array.reshape(lead + (TILES, 8, BLOCKS, 128))
        return jnp.swapaxes(split, n + 1, n + 2)

    f32 = jnp.float32
    whole = (2, TILES, BLOCKS, 8, 128)
    parts = (TILES, 8, 2, 4, 8, 128)
    dma = pltpu.SemaphoreType.DMA
    out, biggest = pl.pallas_call(
        kernel,
        out_shape=(
            pltpu.VMEM(whole, f32),
            jax.ShapeDtypeStruct((1, 1), f32),
        ),
        in_specs=[pl.BlockSpec(memory_space=pltpu.HBM)] * 4,
        out_specs=(pl.BlockSpec(memory_space=pltpu.VMEM), pl.BlockSpec(memory_space=pltpu.SMEM)),
        scratch_shapes=[
            pltpu.VMEM((SWEEPS, 2, BLOCKS, ROWS, 128), f32),
            pltpu.VMEM(whole, f32),
            pltpu.VMEM(whole[1:], f32),
            pltpu.VMEM(whole[1:], f32),
            pltpu.VMEM(parts, f32),
            pltpu.VMEM(parts, f32),
            pltpu.VMEM(parts, f32),
            pltpu.VMEM(parts, f32),
            pltpu.VMEM(parts, f32),
            pltpu.VMEM((TILES + 2, 2, BLOCKS, 8, 128), f32),
            pltpu.VMEM((2, 2, 2, BLOCKS, 8, 128), f32),
            pltpu.VMEM((2, 2, BLOCKS, 128), f32),
            pltpu.VMEM((2, 2, BLOCKS, 128), f32),
            pltpu.VMEM((2, SWEEPS - 1, 2, BLOCKS, 128), f32),
            pltpu.VMEM((2, SWEEPS - 1, 2, BLOCKS, 128), f32),
            pltpu.VMEM((1, 128), f32),
            pltpu.VMEM((32, 1, 128), f32),
            pltpu.VMEM((1, 128), f32),
            pltpu.VMEM((8, 1, 128), f32),
            dma((TILES, 2)),
            dma((TILES, 2)),
            dma,
            dma,
            dma((TILES,)),
            dma,
            dma((TILES,)),
            dma((2,)),
            dma((2,)),
            dma((2,)),
            dma((2,)),
            dma((32,)),
            dma((32,)),
            dma((8,)),
            dma((8,)),
            pltpu.SemaphoreType.REGULAR((2,)),
        ],
        compiler_params=pltpu.CompilerParams(
            collective_id=0, has_side_effects=True, vmem_limit_bytes=44 * 1024 * 1024
        ),
    )(*[pltpu.with_memory_space_constraint(tiled(x), pltpu.HBM) for x in (sections[0], initial, feed_rate, kill_rate)])
    new = jnp.swapaxes(out, 2, 3).reshape(sections.shape)
    return (new, biggest.reshape(()))


def solution(mesh):
    return jax.shard_map(
        shards,
        mesh=mesh,
        in_specs=(
            P(None, "space", None),
            P("node", None, "space", None),
            P("space", None),
            P("space", None),
        ),
        out_specs=(P("node", None, "space", None), P()),
        check_vma=False,
    )
```

```python
import functools

import jax
import jax.numpy as jnp
import numpy as np
from jax import lax
from jax.experimental import pallas as pl
from jax.experimental.pallas import tpu as pltpu
from jax.sharding import PartitionSpec as P

SWEEPS = 6
STEP_SIZE = 4.0
DIFFUSIVITY = (1.0, 0.5)
MESH = pl.DeviceIdType.MESH

TILES = 8
BLOCKS = 32
ROWS = 104
FIRST = 16
ORDER = (1, 6, 0, 7, 5, 4, 3, 2)
GROUP = 16
LAG = 2
AHEAD = 3


def radau_target(order, value):
    before = 1.0
    current = value
    previous = 1.0
    for degree in range(1, order):
        following = ((2 * degree + 1) * value * current - degree * before) / (degree + 1)
        before = current
        current = following
    previous = before
    return current - previous


@functools.lru_cache(maxsize=None)
def radau_table(total):
    grid_count = 20000
    roots_found = []
    left_value = -1.0
    left_target = radau_target(total, left_value)
    for step_index in range(1, grid_count):
        right_value = -1.0 + 2.0 * step_index / grid_count
        right_target = radau_target(total, right_value)
        if left_target * right_target < 0.0:
            lower = left_value
            upper = right_value
            lower_target = left_target
            for _ in range(80):
                halfway = 0.5 * (lower + upper)
                halfway_target = radau_target(total, halfway)
                if lower_target * halfway_target <= 0.0:
                    upper = halfway
                else:
                    lower = halfway
                    lower_target = halfway_target
            roots_found.append(0.5 * (lower + upper))
        left_value = right_value
        left_target = right_target
    roots_found.append(1.0)
    points = [(value + 1.0) / 2.0 for value in roots_found]
    quad_rows = []
    for node_index in range(total):
        row_values = []
        for basis_index in range(total):
            coefs = [1.0]
            for other_index in range(total):
                if other_index != basis_index:
                    scale = 1.0 / (points[basis_index] - points[other_index])
                    shifted = [0.0] + coefs
                    widened = coefs + [0.0]
                    coefs = [
                        (shifted[k] - points[other_index] * widened[k]) * scale
                        for k in range(len(shifted))
                    ]
            integral = 0.0
            for power_index in range(len(coefs)):
                integral += (
                    coefs[power_index] * points[node_index] ** (power_index + 1) / (power_index + 1)
                )
            row_values.append(integral)
        quad_rows.append(row_values)
    return (np.array(points, np.float32), np.array(quad_rows, np.float32))


def kernel(
    sec_hbm, init_hbm, feed_hbm, kill_hbm,
    out, res_out,
    levels, init, feed, kill, slopes, gathered, mixed, summed, drift, right, partial,
    halo_out, halo_in, edge_out, edge_in, top, top_in, best, best_in,
    load_sem, field_sem, init_sem,
    slope_send, slope_recv, mixed_send, mixed_recv,
    halo_send, halo_recv, edge_send, edge_recv,
    top_send, top_recv, best_send, best_recv, known_sem,
):
    node = lax.axis_index("node")
    space = lax.axis_index("space")
    points, quad = radau_table(8)

    def per_node(values):
        chosen = jnp.float32(values[0])
        for index in range(1, 8):
            chosen = jnp.where(node == index, jnp.float32(values[index]), chosen)
        return chosen

    steps = np.float32(STEP_SIZE) * points
    couplings = [steps * np.float32(d) for d in DIFFUSIVITY]
    divisors = [np.float32(4.0) * c + np.float32(1.0) for c in couplings]
    node_step = per_node(steps)
    inverse = [per_node((1.0 / d.astype(np.float64)).astype(np.float32)) for d in divisors]
    ratio = [
        per_node((c.astype(np.float64) / d.astype(np.float64)).astype(np.float32))
        for c, d in zip(couplings, divisors)
    ]

    def node_peer(i):
        y, x = node // 4, node % 4
        return (((y + i // 4) % 2) * 4 + (x + i % 4) % 4, space)

    def node_index(i):
        return node_peer(i)[0]

    def plane_peer(j):
        return (node_index(j % 8), (space // 4) * 4 + (space % 4 + j // 8) % 4)

    def deep_peer(i):
        return (node, (space // 4 + i) % 8 * 4 + space % 4)

    def next_peer(i):
        return (node, (space + i + 32) % 32)

    barrier = pltpu.get_barrier_semaphore()
    greeted = (
        [node_peer(i) for i in range(1, 8)]
        + [plane_peer(8 * i) for i in range(1, 4)]
        + [deep_peer(1), deep_peer(7), next_peer(1), next_peer(-1)]
    )
    loads = []
    for t in range(TILES):
        loads.append([
            pltpu.make_async_copy(
                sec_hbm.at[s, t], levels.at[0, s, :, pl.ds(FIRST + 8 * t, 8), :], load_sem.at[t, s]
            )
            for s in range(2)
        ])
    fields = [
        [
            pltpu.make_async_copy(feed_hbm.at[t], feed.at[t], field_sem.at[t, 0]),
            pltpu.make_async_copy(kill_hbm.at[t], kill.at[t], field_sem.at[t, 1]),
        ]
        for t in range(TILES)
    ]
    init_load = pltpu.make_async_copy(init_hbm, init, init_sem)
    started, waited = set(), set()

    def start_loads(t):
        for near in (t - 1, t, t + 1):
            if 0 <= near < TILES and near not in started:
                started.add(near)
                for copy in loads[near]:
                    copy.start()
        for copy in fields[t]:
            copy.start()

    def wait_loads(t):
        for near in (t - 1, t, t + 1):
            if 0 <= near < TILES and near not in waited:
                waited.add(near)
                for copy in loads[near]:
                    copy.wait()
        for copy in fields[t]:
            copy.wait()

    start_loads(ORDER[0])
    for peer in greeted:
        pl.semaphore_signal(barrier, inc=1, device_id=peer, device_id_type=MESH)
    for t in ORDER[1:]:
        start_loads(t)
    init_load.start()

    lane = lax.broadcasted_iota(jnp.int32, (8, 128), 1)
    row = lax.broadcasted_iota(jnp.int32, (8, 128), 0)

    def beside(before, centre, after):
        left = pltpu.roll(jnp.where(lane == 127, before, centre), 1, 1)
        rightward = pltpu.roll(jnp.where(lane == 0, after, centre), 127, 1)
        return rightward + left

    def centres(load, first, count):
        blocks = [(first + BLOCKS - 1) % BLOCKS]
        blocks += [first + i for i in range(count)]
        blocks += [(first + count) % BLOCKS]
        return [load(b) for b in blocks]

    def slope_tile(t):
        base = FIRST + 8 * t

        def body(d, carry):
            first = d * 4
            found = []
            for s in range(2):
                line = centres(lambda b: levels[0, s, b, pl.ds(base, 8), :], first, 4)
                laps = []
                for q in range(4):
                    up = levels[0, s, first + q, pl.ds(base - 1, 8), :]
                    down = levels[0, s, first + q, pl.ds(base + 1, 8), :]
                    around = (down + up) + beside(line[q], line[q + 1], line[q + 2])
                    laps.append((line[q + 1], around - 4.0 * line[q + 1]))
                found.append(laps)
            for q in range(4):
                u, lap_u = found[0][q]
                v, lap_v = found[1][q]
                lap_v = 0.5 * lap_v
                grow = feed[t, first + q]
                both = grow + kill[t, first + q]
                product = u * v * v
                slopes[t, d, 0, q] = lap_u + (grow * (1.0 - u) - product)
                slopes[t, d, 1, q] = lap_v + (product - both * v)
                drift[t, d, 0, q] = node_step * lap_u
                drift[t, d, 1, q] = node_step * lap_v
            return carry

        lax.fori_loop(0, 8, body, 0)

    def exchange(source, target, t, send_sem, recv_sem):
        copies = []
        for i in range(1, 8):
            copy = pltpu.make_async_remote_copy(
                source.at[t, node_index(i)], target.at[t, node],
                send_sem, recv_sem.at[t], device_id=node_peer(i), device_id_type=MESH,
            )
            copy.start()
        target[t, node] = source[t, node]

    def arrived(target, t, recv_sem):
        part = target.at[t, pl.ds(0, 7)]
        pltpu.make_async_copy(part, part, recv_sem.at[t]).wait()

    def mix_tile(t):
        def body(piece, carry):
            s, q = piece // 4, piece % 4
            values = [gathered[t, j, s, q] for j in range(8)]
            for m in range(8):
                total = values[0] * float(STEP_SIZE * quad[m, 0])
                for j in range(1, 8):
                    total = total + values[j] * float(STEP_SIZE * quad[m, j])
                mixed[t, m, s, q] = total
            return carry

        lax.fori_loop(0, 8, body, 0)

    def right_tile(t, biggest):
        base = FIRST + 8 * t

        def body(d, carry):
            for s in range(2):
                for q in range(4):
                    block = d * 4 + q
                    value = init[s, t, block] + summed[t, d, s, q]
                    here = levels[0, s, block, pl.ds(base, 8), :]
                    carry = jnp.maximum(carry, jnp.abs(value - here))
                    right[t + 1, s, block] = (value - drift[t, d, s, q]) * inverse[s]
            return carry

        return lax.fori_loop(0, 8, body, biggest)

    def sweep(level, t, side=None):
        base = pl.multiple_of(FIRST + 8 * t, 8)
        for s in range(2):
            line = centres(lambda b: levels[level - 1, s, b, pl.ds(base, 8), :], 0, BLOCKS)
            for b in range(BLOCKS):
                up = levels[level - 1, s, b, pl.ds(base - 1, 8), :]
                down = levels[level - 1, s, b, pl.ds(base + 1, 8), :]
                around = (down + up) + beside(line[b], line[b + 1], line[b + 2])
                if side is not None:
                    beyond = jnp.broadcast_to(edge_in[side, level - 2, s, pl.ds(b, 1), :], (8, 128))
                    around = around + jnp.where(row == 7 * side, beyond, 0.0)
                value = right[t + 1, s, b] + ratio[s] * around
                if level == SWEEPS:
                    out[s, t, b] = value
                else:
                    levels[level, s, b, pl.ds(base, 8), :] = value

    def response(level, side):
        base = pl.multiple_of(FIRST - 8 + 72 * side, 8)
        for s in range(2):
            if level == 1:
                for b in range(BLOCKS):
                    near = levels[0, s, b, pl.ds(base + 1 - 2 * side, 8), :]
                    levels[1, s, b, pl.ds(base, 8), :] = jnp.where(
                        row == 7 - 7 * side, ratio[s] * near, 0.0
                    )
                continue
            line = centres(lambda b: levels[level - 1, s, b, pl.ds(base, 8), :], 0, BLOCKS)
            for b in range(BLOCKS):
                up = levels[level - 1, s, b, pl.ds(base - 1, 8), :]
                down = levels[level - 1, s, b, pl.ds(base + 1, 8), :]
                around = (down + up) + beside(line[b], line[b + 1], line[b + 2])
                levels[level, s, b, pl.ds(base, 8), :] = ratio[s] * around

    def repeat(low, high, run):
        def body(t, carry):
            run(t)
            return carry

        lax.fori_loop(low, high, body, 0)

    def sweep_all(low, high, last_low, last_high):
        for level in range(1, SWEEPS):
            repeat(low, high, functools.partial(sweep, level))
        if last_high > last_low:
            repeat(last_low, last_high, functools.partial(sweep, SWEEPS))

    def send_edges():
        for e, t in ((0, 0), (1, 7)):
            for s in range(2):
                for k in range(1, SWEEPS):
                    def body(g, carry):
                        first = g * GROUP
                        if k == 1:
                            load = lambda b: levels[0, s, b, pl.ds(FIRST + 8 * t, 8), :]
                        else:
                            load = lambda b: partial[(k - 1) % 2, e, s, b]
                        line = centres(load, first, GROUP)
                        for i in range(GROUP):
                            centre = line[i + 1]
                            up = jnp.where(row == 0, 0.0, pltpu.roll(centre, 1, 0))
                            down = jnp.where(row == 7, 0.0, pltpu.roll(centre, 7, 0))
                            around = (down + up) + beside(line[i], centre, line[i + 2])
                            partial[k % 2, e, s, first + i] = (
                                right[t + 1, s, first + i] + ratio[s] * around
                            )
                        return carry

                    lax.fori_loop(0, BLOCKS // GROUP, body, 0)
                    flat = partial.at[k % 2, e, s].reshape(BLOCKS * 8, 128)
                    edge_out[e, k - 1, s] = flat[pl.ds(7 * e, BLOCKS, stride=8), :]

    def side_copies(source, target, send_sem, recv_sem):
        return [
            pltpu.make_async_remote_copy(
                source.at[e], target.at[1 - e], send_sem.at[e], recv_sem.at[1 - e],
                device_id=next_peer(2 * e - 1), device_id_type=MESH,
            )
            for e in range(2)
        ]

    halo_copies = side_copies(halo_out, halo_in, halo_send, halo_recv)
    edge_copies = side_copies(edge_out, edge_in, edge_send, edge_recv)

    wait_loads(ORDER[0])
    slope_tile(ORDER[0])
    pl.semaphore_wait(barrier, len(greeted))
    exchange(slopes, gathered, ORDER[0], slope_send, slope_recv)
    wait_loads(ORDER[1])
    for s in range(2):
        flat = levels.at[0, s].reshape(BLOCKS * ROWS, 128)
        halo_out[0, s] = flat[pl.ds(FIRST, BLOCKS, stride=ROWS), :]
        halo_out[1, s] = flat[pl.ds(FIRST + 63, BLOCKS, stride=ROWS), :]
    for copy in halo_copies:
        copy.start()
    for peer in [plane_peer(8 * i) for i in range(1, 4)] + [deep_peer(1), deep_peer(7)]:
        pl.semaphore_signal(known_sem.at[0], inc=1, device_id=peer, device_id_type=MESH)
    slope_tile(ORDER[1])
    exchange(slopes, gathered, ORDER[1], slope_send, slope_recv)
    for copy in halo_copies:
        copy.wait_recv()
    for s in range(2):
        flat = levels.at[0, s].reshape(BLOCKS * ROWS, 128)
        flat[pl.ds(FIRST - 1, BLOCKS, stride=ROWS), :] = halo_in[0, s]
        flat[pl.ds(FIRST + 64, BLOCKS, stride=ROWS), :] = halo_in[1, s]
    def send_slopes(t):
        wait_loads(t)
        slope_tile(t)
        exchange(slopes, gathered, t, slope_send, slope_recv)

    for t in ORDER[2:AHEAD]:
        send_slopes(t)
    pl.semaphore_wait(known_sem.at[0], 5)
    for i in (2, 6):
        pl.semaphore_signal(known_sem.at[1], inc=1, device_id=deep_peer(i), device_id_type=MESH)

    init_load.wait()
    biggest = jnp.zeros((8, 128), jnp.float32)
    for step in range(TILES + LAG):
        if step < TILES:
            t = ORDER[step]
            arrived(gathered, t, slope_recv)
            mix_tile(t)
            exchange(mixed, summed, t, mixed_send, mixed_recv)
            if step + AHEAD < TILES:
                send_slopes(ORDER[step + AHEAD])
        index = step - LAG
        if index < 0:
            continue
        t = ORDER[index]
        arrived(summed, t, mixed_recv)
        if index == 6:
            for copy in edge_copies:
                copy.start()
        biggest = right_tile(t, biggest)
        if index == 2:
            sweep_all(0, 2, 0, 0)
        if index == 3:
            send_edges()
        if index == 4:
            sweep_all(5, 8, 6, 7)
        if index == 5:
            sweep_all(4, 6, 5, 6)
        if index == 6:
            sweep_all(3, 5, 4, 5)
    pl.semaphore_wait(known_sem.at[1], 2)

    top[...] = jnp.max(biggest, axis=0, keepdims=True)
    top_copies = []
    for j in range(1, 32):
        copy = pltpu.make_async_remote_copy(
            top, top_in.at[j], top_send.at[j], top_recv.at[j],
            device_id=plane_peer(j), device_id_type=MESH,
        )
        copy.start()
        top_copies.append(copy)
    top_in[0] = top[...]

    sweep_all(1, 4, 1, 4)

    for copy in top_copies:
        copy.wait_recv()
    best[...] = jnp.max(top_in[...], axis=0)
    best_copies = []
    for i in range(1, 8):
        copy = pltpu.make_async_remote_copy(
            best, best_in.at[i], best_send.at[i], best_recv.at[i],
            device_id=deep_peer(i), device_id_type=MESH,
        )
        copy.start()
        best_copies.append(copy)
    best_in[0] = best[...]

    for copy in edge_copies:
        copy.wait_recv()
    for level in range(1, SWEEPS + 1):
        if level > 1:
            repeat(0, 2, lambda side: sweep(level, 7 * side, side))
        if level < SWEEPS:
            repeat(0, 2, functools.partial(response, level))

    for copy in best_copies:
        copy.wait_recv()
    res_out[0, 0] = jnp.max(best_in[...])

    for source, sem in ((slopes, slope_send), (mixed, mixed_send)):
        part = source.at[:, pl.ds(0, 7)]
        pltpu.make_async_copy(part, part, sem).wait()
    for copy in halo_copies + edge_copies + top_copies + best_copies:
        copy.wait_send()


def shards(initial, sections, feed_rate, kill_rate):
    def tiled(array):
        lead = array.shape[:-2]
        n = len(lead)
        split = array.reshape(lead + (TILES, 8, BLOCKS, 128))
        return jnp.swapaxes(split, n + 1, n + 2)

    f32 = jnp.float32
    whole = (2, TILES, BLOCKS, 8, 128)
    parts = (TILES, 8, 2, 4, 8, 128)
    dma = pltpu.SemaphoreType.DMA
    out, biggest = pl.pallas_call(
        kernel,
        out_shape=(
            pltpu.VMEM(whole, f32),
            jax.ShapeDtypeStruct((1, 1), f32),
        ),
        in_specs=[pl.BlockSpec(memory_space=pltpu.HBM)] * 4,
        out_specs=(pl.BlockSpec(memory_space=pltpu.VMEM), pl.BlockSpec(memory_space=pltpu.SMEM)),
        scratch_shapes=[
            pltpu.VMEM((SWEEPS, 2, BLOCKS, ROWS, 128), f32),
            pltpu.VMEM(whole, f32),
            pltpu.VMEM(whole[1:], f32),
            pltpu.VMEM(whole[1:], f32),
            pltpu.VMEM(parts, f32),
            pltpu.VMEM(parts, f32),
            pltpu.VMEM(parts, f32),
            pltpu.VMEM(parts, f32),
            pltpu.VMEM(parts, f32),
            pltpu.VMEM((TILES + 2, 2, BLOCKS, 8, 128), f32),
            pltpu.VMEM((2, 2, 2, BLOCKS, 8, 128), f32),
            pltpu.VMEM((2, 2, BLOCKS, 128), f32),
            pltpu.VMEM((2, 2, BLOCKS, 128), f32),
            pltpu.VMEM((2, SWEEPS - 1, 2, BLOCKS, 128), f32),
            pltpu.VMEM((2, SWEEPS - 1, 2, BLOCKS, 128), f32),
            pltpu.VMEM((1, 128), f32),
            pltpu.VMEM((32, 1, 128), f32),
            pltpu.VMEM((1, 128), f32),
            pltpu.VMEM((8, 1, 128), f32),
            dma((TILES, 2)),
            dma((TILES, 2)),
            dma,
            dma,
            dma((TILES,)),
            dma,
            dma((TILES,)),
            dma((2,)),
            dma((2,)),
            dma((2,)),
            dma((2,)),
            dma((32,)),
            dma((32,)),
            dma((8,)),
            dma((8,)),
            pltpu.SemaphoreType.REGULAR((2,)),
        ],
        compiler_params=pltpu.CompilerParams(
            collective_id=0, has_side_effects=True, vmem_limit_bytes=44 * 1024 * 1024
        ),
    )(*[pltpu.with_memory_space_constraint(tiled(x), pltpu.HBM) for x in (sections[0], initial, feed_rate, kill_rate)])
    new = jnp.swapaxes(out, 2, 3).reshape(sections.shape)
    return (new, biggest.reshape(()))


def solution(mesh):
    return jax.shard_map(
        shards,
        mesh=mesh,
        in_specs=(
            P(None, "space", None),
            P("node", None, "space", None),
            P("space", None),
            P("space", None),
        ),
        out_specs=(P("node", None, "space", None), P()),
        check_vma=False,
    )
```

```python
import functools

import jax
import jax.numpy as jnp
import numpy as np
from jax import lax
from jax.experimental import pallas as pl
from jax.experimental.pallas import tpu as pltpu
from jax.sharding import PartitionSpec as P

SWEEPS = 6
STEP_SIZE = 4.0
DIFFUSIVITY = (1.0, 0.5)
MESH = pl.DeviceIdType.MESH

TILES = 8
BLOCKS = 32
ROWS = 104
FIRST = 16
ORDER = (1, 6, 0, 7, 5, 4, 3, 2)
GROUP = 32
LAG = 2
AHEAD = 3


def radau_target(order, value):
    before = 1.0
    current = value
    previous = 1.0
    for degree in range(1, order):
        following = ((2 * degree + 1) * value * current - degree * before) / (degree + 1)
        before = current
        current = following
    previous = before
    return current - previous


@functools.lru_cache(maxsize=None)
def radau_table(total):
    grid_count = 20000
    roots_found = []
    left_value = -1.0
    left_target = radau_target(total, left_value)
    for step_index in range(1, grid_count):
        right_value = -1.0 + 2.0 * step_index / grid_count
        right_target = radau_target(total, right_value)
        if left_target * right_target < 0.0:
            lower = left_value
            upper = right_value
            lower_target = left_target
            for _ in range(80):
                halfway = 0.5 * (lower + upper)
                halfway_target = radau_target(total, halfway)
                if lower_target * halfway_target <= 0.0:
                    upper = halfway
                else:
                    lower = halfway
                    lower_target = halfway_target
            roots_found.append(0.5 * (lower + upper))
        left_value = right_value
        left_target = right_target
    roots_found.append(1.0)
    points = [(value + 1.0) / 2.0 for value in roots_found]
    quad_rows = []
    for node_index in range(total):
        row_values = []
        for basis_index in range(total):
            coefs = [1.0]
            for other_index in range(total):
                if other_index != basis_index:
                    scale = 1.0 / (points[basis_index] - points[other_index])
                    shifted = [0.0] + coefs
                    widened = coefs + [0.0]
                    coefs = [
                        (shifted[k] - points[other_index] * widened[k]) * scale
                        for k in range(len(shifted))
                    ]
            integral = 0.0
            for power_index in range(len(coefs)):
                integral += (
                    coefs[power_index] * points[node_index] ** (power_index + 1) / (power_index + 1)
                )
            row_values.append(integral)
        quad_rows.append(row_values)
    return (np.array(points, np.float32), np.array(quad_rows, np.float32))


def kernel(
    sec_hbm, init_hbm, feed_hbm, kill_hbm,
    out, res_out,
    levels, init, feed, kill, slopes, gathered, mixed, summed, drift, right, partial,
    halo_out, halo_in, edge_out, edge_in, top, top_in, best, best_in,
    load_sem, field_sem, init_sem,
    slope_send, slope_recv, mixed_send, mixed_recv,
    halo_send, halo_recv, edge_send, edge_recv,
    top_send, top_recv, best_send, best_recv, known_sem,
):
    node = lax.axis_index("node")
    space = lax.axis_index("space")
    points, quad = radau_table(8)

    def per_node(values):
        chosen = jnp.float32(values[0])
        for index in range(1, 8):
            chosen = jnp.where(node == index, jnp.float32(values[index]), chosen)
        return chosen

    steps = np.float32(STEP_SIZE) * points
    couplings = [steps * np.float32(d) for d in DIFFUSIVITY]
    divisors = [np.float32(4.0) * c + np.float32(1.0) for c in couplings]
    node_step = per_node(steps)
    inverse = [per_node((1.0 / d.astype(np.float64)).astype(np.float32)) for d in divisors]
    ratio = [
        per_node((c.astype(np.float64) / d.astype(np.float64)).astype(np.float32))
        for c, d in zip(couplings, divisors)
    ]

    def node_peer(i):
        y, x = node // 4, node % 4
        return (((y + i // 4) % 2) * 4 + (x + i % 4) % 4, space)

    def node_index(i):
        return node_peer(i)[0]

    def plane_peer(j):
        return (node_index(j % 8), (space // 4) * 4 + (space % 4 + j // 8) % 4)

    def deep_peer(i):
        return (node, (space // 4 + i) % 8 * 4 + space % 4)

    def next_peer(i):
        return (node, (space + i + 32) % 32)

    barrier = pltpu.get_barrier_semaphore()
    greeted = (
        [node_peer(i) for i in range(1, 8)]
        + [plane_peer(8 * i) for i in range(1, 4)]
        + [deep_peer(1), deep_peer(7), next_peer(1), next_peer(-1)]
    )
    loads = []
    for t in range(TILES):
        loads.append([
            pltpu.make_async_copy(
                sec_hbm.at[s, t], levels.at[0, s, :, pl.ds(FIRST + 8 * t, 8), :], load_sem.at[t, s]
            )
            for s in range(2)
        ])
    fields = [
        [
            pltpu.make_async_copy(feed_hbm.at[t], feed.at[t], field_sem.at[t, 0]),
            pltpu.make_async_copy(kill_hbm.at[t], kill.at[t], field_sem.at[t, 1]),
        ]
        for t in range(TILES)
    ]
    init_load = pltpu.make_async_copy(init_hbm, init, init_sem)
    started, waited = set(), set()

    def start_loads(t):
        for near in (t - 1, t, t + 1):
            if 0 <= near < TILES and near not in started:
                started.add(near)
                for copy in loads[near]:
                    copy.start()
        for copy in fields[t]:
            copy.start()

    def wait_loads(t):
        for near in (t - 1, t, t + 1):
            if 0 <= near < TILES and near not in waited:
                waited.add(near)
                for copy in loads[near]:
                    copy.wait()
        for copy in fields[t]:
            copy.wait()

    start_loads(ORDER[0])
    for peer in greeted:
        pl.semaphore_signal(barrier, inc=1, device_id=peer, device_id_type=MESH)
    for t in ORDER[1:]:
        start_loads(t)
    init_load.start()

    lane = lax.broadcasted_iota(jnp.int32, (8, 128), 1)
    row = lax.broadcasted_iota(jnp.int32, (8, 128), 0)

    def beside(before, centre, after):
        left = pltpu.roll(jnp.where(lane == 127, before, centre), 1, 1)
        rightward = pltpu.roll(jnp.where(lane == 0, after, centre), 127, 1)
        return rightward + left

    def centres(load, first, count):
        blocks = [(first + BLOCKS - 1) % BLOCKS]
        blocks += [first + i for i in range(count)]
        blocks += [(first + count) % BLOCKS]
        return [load(b) for b in blocks]

    def slope_tile(t):
        base = FIRST + 8 * t

        def body(d, carry):
            first = d * 4
            found = []
            for s in range(2):
                line = centres(lambda b: levels[0, s, b, pl.ds(base, 8), :], first, 4)
                laps = []
                for q in range(4):
                    up = levels[0, s, first + q, pl.ds(base - 1, 8), :]
                    down = levels[0, s, first + q, pl.ds(base + 1, 8), :]
                    around = (down + up) + beside(line[q], line[q + 1], line[q + 2])
                    laps.append((line[q + 1], around - 4.0 * line[q + 1]))
                found.append(laps)
            for q in range(4):
                u, lap_u = found[0][q]
                v, lap_v = found[1][q]
                lap_v = 0.5 * lap_v
                grow = feed[t, first + q]
                both = grow + kill[t, first + q]
                product = u * v * v
                slopes[t, d, 0, q] = lap_u + (grow * (1.0 - u) - product)
                slopes[t, d, 1, q] = lap_v + (product - both * v)
                drift[t, d, 0, q] = node_step * lap_u
                drift[t, d, 1, q] = node_step * lap_v
            return carry

        lax.fori_loop(0, 8, body, 0)

    def exchange(source, target, t, send_sem, recv_sem):
        copies = []
        for i in range(1, 8):
            copy = pltpu.make_async_remote_copy(
                source.at[t, node_index(i)], target.at[t, node],
                send_sem, recv_sem.at[t], device_id=node_peer(i), device_id_type=MESH,
            )
            copy.start()
        target[t, node] = source[t, node]

    def arrived(target, t, recv_sem):
        part = target.at[t, pl.ds(0, 7)]
        pltpu.make_async_copy(part, part, recv_sem.at[t]).wait()

    def mix_tile(t):
        def body(piece, carry):
            s, q = piece // 4, piece % 4
            values = [gathered[t, j, s, q] for j in range(8)]
            for m in range(8):
                total = values[0] * float(STEP_SIZE * quad[m, 0])
                for j in range(1, 8):
                    total = total + values[j] * float(STEP_SIZE * quad[m, j])
                mixed[t, m, s, q] = total
            return carry

        lax.fori_loop(0, 8, body, 0)

    def right_tile(t, biggest):
        base = FIRST + 8 * t

        def body(d, carry):
            for s in range(2):
                for q in range(4):
                    block = d * 4 + q
                    value = init[s, t, block] + summed[t, d, s, q]
                    here = levels[0, s, block, pl.ds(base, 8), :]
                    carry = jnp.maximum(carry, jnp.abs(value - here))
                    right[t + 1, s, block] = (value - drift[t, d, s, q]) * inverse[s]
            return carry

        return lax.fori_loop(0, 8, body, biggest)

    def sweep(level, t, side=None):
        base = pl.multiple_of(FIRST + 8 * t, 8)
        for s in range(2):
            line = centres(lambda b: levels[level - 1, s, b, pl.ds(base, 8), :], 0, BLOCKS)
            for b in range(BLOCKS):
                up = levels[level - 1, s, b, pl.ds(base - 1, 8), :]
                down = levels[level - 1, s, b, pl.ds(base + 1, 8), :]
                around = (down + up) + beside(line[b], line[b + 1], line[b + 2])
                if side is not None:
                    beyond = jnp.broadcast_to(edge_in[side, level - 2, s, pl.ds(b, 1), :], (8, 128))
                    around = around + jnp.where(row == 7 * side, beyond, 0.0)
                value = right[t + 1, s, b] + ratio[s] * around
                if level == SWEEPS:
                    out[s, t, b] = value
                else:
                    levels[level, s, b, pl.ds(base, 8), :] = value

    def response(level, side):
        base = pl.multiple_of(FIRST - 8 + 72 * side, 8)
        for s in range(2):
            if level == 1:
                for b in range(BLOCKS):
                    near = levels[0, s, b, pl.ds(base + 1 - 2 * side, 8), :]
                    levels[1, s, b, pl.ds(base, 8), :] = jnp.where(
                        row == 7 - 7 * side, ratio[s] * near, 0.0
                    )
                continue
            line = centres(lambda b: levels[level - 1, s, b, pl.ds(base, 8), :], 0, BLOCKS)
            for b in range(BLOCKS):
                up = levels[level - 1, s, b, pl.ds(base - 1, 8), :]
                down = levels[level - 1, s, b, pl.ds(base + 1, 8), :]
                around = (down + up) + beside(line[b], line[b + 1], line[b + 2])
                levels[level, s, b, pl.ds(base, 8), :] = ratio[s] * around

    def repeat(low, high, run):
        def body(t, carry):
            run(t)
            return carry

        lax.fori_loop(low, high, body, 0)

    def sweep_all(low, high, last_low, last_high):
        for level in range(1, SWEEPS):
            repeat(low, high, functools.partial(sweep, level))
        if last_high > last_low:
            repeat(last_low, last_high, functools.partial(sweep, SWEEPS))

    def send_edges():
        for e, t in ((0, 0), (1, 7)):
            for s in range(2):
                for k in range(1, SWEEPS):
                    def body(g, carry):
                        first = g * GROUP
                        if k == 1:
                            load = lambda b: levels[0, s, b, pl.ds(FIRST + 8 * t, 8), :]
                        else:
                            load = lambda b: partial[(k - 1) % 2, e, s, b]
                        line = centres(load, first, GROUP)
                        for i in range(GROUP):
                            centre = line[i + 1]
                            up = jnp.where(row == 0, 0.0, pltpu.roll(centre, 1, 0))
                            down = jnp.where(row == 7, 0.0, pltpu.roll(centre, 7, 0))
                            around = (down + up) + beside(line[i], centre, line[i + 2])
                            partial[k % 2, e, s, first + i] = (
                                right[t + 1, s, first + i] + ratio[s] * around
                            )
                        return carry

                    lax.fori_loop(0, BLOCKS // GROUP, body, 0)
                    flat = partial.at[k % 2, e, s].reshape(BLOCKS * 8, 128)
                    edge_out[e, k - 1, s] = flat[pl.ds(7 * e, BLOCKS, stride=8), :]

    def side_copies(source, target, send_sem, recv_sem):
        return [
            pltpu.make_async_remote_copy(
                source.at[e], target.at[1 - e], send_sem.at[e], recv_sem.at[1 - e],
                device_id=next_peer(2 * e - 1), device_id_type=MESH,
            )
            for e in range(2)
        ]

    halo_copies = side_copies(halo_out, halo_in, halo_send, halo_recv)
    edge_copies = side_copies(edge_out, edge_in, edge_send, edge_recv)

    wait_loads(ORDER[0])
    slope_tile(ORDER[0])
    pl.semaphore_wait(barrier, len(greeted))
    exchange(slopes, gathered, ORDER[0], slope_send, slope_recv)
    wait_loads(ORDER[1])
    for s in range(2):
        flat = levels.at[0, s].reshape(BLOCKS * ROWS, 128)
        halo_out[0, s] = flat[pl.ds(FIRST, BLOCKS, stride=ROWS), :]
        halo_out[1, s] = flat[pl.ds(FIRST + 63, BLOCKS, stride=ROWS), :]
    for copy in halo_copies:
        copy.start()
    for peer in [plane_peer(8 * i) for i in range(1, 4)] + [deep_peer(1), deep_peer(7)]:
        pl.semaphore_signal(known_sem.at[0], inc=1, device_id=peer, device_id_type=MESH)
    slope_tile(ORDER[1])
    exchange(slopes, gathered, ORDER[1], slope_send, slope_recv)
    for copy in halo_copies:
        copy.wait_recv()
    for s in range(2):
        flat = levels.at[0, s].reshape(BLOCKS * ROWS, 128)
        flat[pl.ds(FIRST - 1, BLOCKS, stride=ROWS), :] = halo_in[0, s]
        flat[pl.ds(FIRST + 64, BLOCKS, stride=ROWS), :] = halo_in[1, s]
    def send_slopes(t):
        wait_loads(t)
        slope_tile(t)
        exchange(slopes, gathered, t, slope_send, slope_recv)

    for t in ORDER[2:AHEAD]:
        send_slopes(t)
    pl.semaphore_wait(known_sem.at[0], 5)
    for i in (2, 6):
        pl.semaphore_signal(known_sem.at[1], inc=1, device_id=deep_peer(i), device_id_type=MESH)

    init_load.wait()
    biggest = jnp.zeros((8, 128), jnp.float32)
    for step in range(TILES + LAG):
        if step < TILES:
            t = ORDER[step]
            arrived(gathered, t, slope_recv)
            mix_tile(t)
            exchange(mixed, summed, t, mixed_send, mixed_recv)
            if step + AHEAD < TILES:
                send_slopes(ORDER[step + AHEAD])
        index = step - LAG
        if index < 0:
            continue
        t = ORDER[index]
        arrived(summed, t, mixed_recv)
        if index == 6:
            for copy in edge_copies:
                copy.start()
        biggest = right_tile(t, biggest)
        if index == 2:
            sweep_all(0, 2, 0, 0)
        if index == 3:
            send_edges()
        if index == 4:
            sweep_all(5, 8, 6, 7)
        if index == 5:
            sweep_all(4, 6, 5, 6)
        if index == 6:
            sweep_all(3, 5, 4, 5)
    pl.semaphore_wait(known_sem.at[1], 2)

    top[...] = jnp.max(biggest, axis=0, keepdims=True)
    top_copies = []
    for j in range(1, 32):
        copy = pltpu.make_async_remote_copy(
            top, top_in.at[j], top_send.at[j], top_recv.at[j],
            device_id=plane_peer(j), device_id_type=MESH,
        )
        copy.start()
        top_copies.append(copy)
    top_in[0] = top[...]

    sweep_all(1, 4, 1, 4)

    for copy in top_copies:
        copy.wait_recv()
    best[...] = jnp.max(top_in[...], axis=0)
    best_copies = []
    for i in range(1, 8):
        copy = pltpu.make_async_remote_copy(
            best, best_in.at[i], best_send.at[i], best_recv.at[i],
            device_id=deep_peer(i), device_id_type=MESH,
        )
        copy.start()
        best_copies.append(copy)
    best_in[0] = best[...]

    for copy in edge_copies:
        copy.wait_recv()
    for level in range(1, SWEEPS + 1):
        if level > 1:
            repeat(0, 2, lambda side: sweep(level, 7 * side, side))
        if level < SWEEPS:
            repeat(0, 2, functools.partial(response, level))

    for copy in best_copies:
        copy.wait_recv()
    res_out[0, 0] = jnp.max(best_in[...])

    for source, sem in ((slopes, slope_send), (mixed, mixed_send)):
        part = source.at[:, pl.ds(0, 7)]
        pltpu.make_async_copy(part, part, sem).wait()
    for copy in halo_copies + edge_copies + top_copies + best_copies:
        copy.wait_send()


def shards(initial, sections, feed_rate, kill_rate):
    def tiled(array):
        lead = array.shape[:-2]
        n = len(lead)
        split = array.reshape(lead + (TILES, 8, BLOCKS, 128))
        return jnp.swapaxes(split, n + 1, n + 2)

    f32 = jnp.float32
    whole = (2, TILES, BLOCKS, 8, 128)
    parts = (TILES, 8, 2, 4, 8, 128)
    dma = pltpu.SemaphoreType.DMA
    out, biggest = pl.pallas_call(
        kernel,
        out_shape=(
            pltpu.VMEM(whole, f32),
            jax.ShapeDtypeStruct((1, 1), f32),
        ),
        in_specs=[pl.BlockSpec(memory_space=pltpu.HBM)] * 4,
        out_specs=(pl.BlockSpec(memory_space=pltpu.VMEM), pl.BlockSpec(memory_space=pltpu.SMEM)),
        scratch_shapes=[
            pltpu.VMEM((SWEEPS, 2, BLOCKS, ROWS, 128), f32),
            pltpu.VMEM(whole, f32),
            pltpu.VMEM(whole[1:], f32),
            pltpu.VMEM(whole[1:], f32),
            pltpu.VMEM(parts, f32),
            pltpu.VMEM(parts, f32),
            pltpu.VMEM(parts, f32),
            pltpu.VMEM(parts, f32),
            pltpu.VMEM(parts, f32),
            pltpu.VMEM((TILES + 2, 2, BLOCKS, 8, 128), f32),
            pltpu.VMEM((2, 2, 2, BLOCKS, 8, 128), f32),
            pltpu.VMEM((2, 2, BLOCKS, 128), f32),
            pltpu.VMEM((2, 2, BLOCKS, 128), f32),
            pltpu.VMEM((2, SWEEPS - 1, 2, BLOCKS, 128), f32),
            pltpu.VMEM((2, SWEEPS - 1, 2, BLOCKS, 128), f32),
            pltpu.VMEM((1, 128), f32),
            pltpu.VMEM((32, 1, 128), f32),
            pltpu.VMEM((1, 128), f32),
            pltpu.VMEM((8, 1, 128), f32),
            dma((TILES, 2)),
            dma((TILES, 2)),
            dma,
            dma,
            dma((TILES,)),
            dma,
            dma((TILES,)),
            dma((2,)),
            dma((2,)),
            dma((2,)),
            dma((2,)),
            dma((32,)),
            dma((32,)),
            dma((8,)),
            dma((8,)),
            pltpu.SemaphoreType.REGULAR((2,)),
        ],
        compiler_params=pltpu.CompilerParams(
            collective_id=0, has_side_effects=True, vmem_limit_bytes=44 * 1024 * 1024
        ),
    )(*[pltpu.with_memory_space_constraint(tiled(x), pltpu.HBM) for x in (sections[0], initial, feed_rate, kill_rate)])
    new = jnp.swapaxes(out, 2, 3).reshape(sections.shape)
    return (new, biggest.reshape(()))


def solution(mesh):
    return jax.shard_map(
        shards,
        mesh=mesh,
        in_specs=(
            P(None, "space", None),
            P("node", None, "space", None),
            P("space", None),
            P("space", None),
        ),
        out_specs=(P("node", None, "space", None), P()),
        check_vma=False,
    )
```
